32 devices in a mesh: gx: 8 (over z, y), gy: 4 (over x, core).
Axes of the slice: x: 2, y: 2, z: 4, core: 2. Of those that a mesh axis runs over, the one named last changes fastest.
Arguments:
- state: float32 [4, 2, 4194304], P('gy', None, 'gx'), may hold values from -6 to 6
- fields: float32 [22], replicated, may hold values from 0.5 to 2
- couplings: float32 [22], replicated, may hold values from 0.5 to 2
- noise: float32 [4, 4, 2], P('gy'), may hold values from -5 to 5
Outputs:
- final_state: float32 [4, 2, 4194304], P('gy', None, 'gx')
- record: float32 [4, 2], replicated
The draws below stay inside these ranges and needn't reach their ends.
All inputs are finite; a program needn't handle non-finite values.
Results may differ from the reference program's by a relative error of at most 0.0001.
Values sent between devices are 32-bit elements; how exact they have to be, the bound alone decides.
A program may use at most 128 MiB of HBM per device.

```python
import math
import jax
import jax.numpy as jnp
from jax import lax

NQ = 22
STEPS = 4
TRAJ = 4
DIM = 4194304


def block_levels(rng, dims, pieces, low, top_value):
    loudness, own = 1.0, jax.random.fold_in(rng, 6)
    for dim, blocks in pieces:
        steps = jnp.exp(jax.random.uniform(jax.random.fold_in(own, dim), (blocks,), jnp.float32, low / len(pieces), top_value / len(pieces)))
        loudness = loudness * jnp.repeat(steps, dims[dim] // blocks).reshape([-1 if axis == dim else 1 for axis in range(len(dims))])
    return loudness


def bell_draw(stream_key, shape, scale, limit, shards=(), kind=jnp.bfloat16):
    gain = block_levels(stream_key, shape, shards, -0.22, 0.18) if shards else 1.0
    values = jax.random.normal(stream_key, shape, jnp.float32) * scale * gain
    return jnp.minimum(jnp.maximum(values, -limit), limit).astype(kind)


def setup_inputs(seed: int = 0) -> dict:
    key_of = jax.random.split(jax.random.key(seed), 5)
    return {
        "state": bell_draw(key_of[0], (TRAJ, 2, DIM), 1.0, 6.0, ((0, 4), (2, 8)), jnp.float32),
        "fields": jnp.clip(jnp.exp(jax.random.uniform(key_of[1], (NQ,), jnp.float32, math.log(0.5), math.log(2.0))), 0.5, 2.0),
        "couplings": jnp.clip(jnp.exp(jax.random.uniform(key_of[2], (NQ,), jnp.float32, math.log(0.5), math.log(2.0))), 0.5, 2.0),
        "noise": bell_draw(key_of[3], (TRAJ, STEPS, 2), 1.0, 5.0, ((0, 4),), jnp.float32),
    }


kappa_rate = 4.0
time_step = 0.05

def flip_qubit(amplitudes, qubit):
    shape = amplitudes.shape
    viewed = amplitudes.reshape(shape[0], shape[1], shape[2] >> qubit + 1, 2, 1 << qubit)
    return jnp.flip(viewed, 3).reshape(shape)

def reference(state, fields, couplings, noise):
    dim_total = state.shape[2]
    count_qubits = dim_total.bit_length() - 1
    position = lax.iota(jnp.int32, dim_total)
    spin_list = [1.0 - 2.0 * (position >> q & 1).astype(jnp.float32) for q in range(count_qubits)]
    occupancy = jnp.zeros((dim_total,), jnp.float32)
    energy = jnp.zeros((dim_total,), jnp.float32)
    for q in range(count_qubits):
        occupancy = occupancy + 0.5 * (1.0 - spin_list[q])
        energy = energy + couplings[q] * spin_list[q] * spin_list[(q + 1) % count_qubits]
    occupancy = occupancy / count_qubits
    amplitudes = state
    records = []
    half_root = jnp.sqrt(jnp.float32(time_step / 2.0))
    for step_id in range(noise.shape[1]):
        weight = amplitudes[:, 0] ** 2 + amplitudes[:, 1] ** 2
        norm_sum = lax.optimization_barrier(jnp.sum(weight, axis=1))
        magnet = lax.optimization_barrier(jnp.sum(weight * occupancy[None, :], axis=1)) / norm_sum
        amplitudes = amplitudes * jnp.sqrt(dim_total / norm_sum)[:, None, None]
        flipped = jnp.zeros_like(amplitudes)
        for q in range(count_qubits):
            flipped = flipped + fields[q] * flip_qubit(amplitudes, q)
        hamil = -flipped - energy[None, None, :] * amplitudes
        shift = occupancy[None, :] - magnet[:, None]
        first = (noise[:, step_id, 0] * half_root)[:, None]
        second = (noise[:, step_id, 1] * half_root)[:, None]
        real_part = amplitudes[:, 0]
        imag_part = amplitudes[:, 1]
        damping = time_step * kappa_rate * 0.5 * shift * shift
        kick = jnp.sqrt(jnp.float32(kappa_rate)) * shift
        new_real = real_part + time_step * hamil[:, 1] - damping * real_part + kick * (real_part * first - imag_part * second)
        new_imag = imag_part - time_step * hamil[:, 0] - damping * imag_part + kick * (real_part * second + imag_part * first)
        amplitudes = jnp.stack([new_real, new_imag], axis=1)
        drift = jnp.sqrt(jnp.float32(kappa_rate)) * magnet * time_step
        both = jnp.stack([drift + first[:, 0], drift + second[:, 0]], axis=1)
        records.append(lax.optimization_barrier(jnp.sum(both, axis=0)))
    return (amplitudes, jnp.stack(records))
```

```python
import functools

import jax
import jax.numpy as jnp
from jax import lax
from jax.experimental import pallas as pl
from jax.experimental.pallas import tpu as pltpu
from jax.sharding import PartitionSpec as P

kappa_rate = 4.0
time_step = 0.05
LANES = 128
CHUNK = 64


def bit_spin(ids, q):
    return 1.0 - 2.0 * (ids >> q & 1).astype(jnp.float32)


def step_kernel(
    high_bits, spins, table, params, block_params, fields, flips, low_energy, own, *rest
):
    partners = rest[:high_bits]
    out, sums = rest[high_bits:]
    rows = own.shape[2]
    row_bits = rows.bit_length() - 1
    chunk_bits = CHUNK.bit_length() - 1
    g = pl.program_id(0)
    rate, factor, damp, kick_one, kick_two, magnet = (params[k] for k in range(6))
    high_ones, top_link, lane_link, high_energy = (block_params[g * 4 + k] for k in range(4))

    row_ids = lax.broadcasted_iota(jnp.int32, (CHUNK, LANES), 0)
    lane_ids = lax.broadcasted_iota(jnp.int32, (CHUNK, LANES), 1)
    ones = jnp.zeros((CHUNK, LANES), jnp.int32)
    for k in range(7):
        ones = ones + (lane_ids >> k & 1)
    for k in range(chunk_bits):
        ones = ones + (row_ids >> k & 1)
    inner_ones = ones.astype(jnp.float32) * (1.0 / spins)
    lane_row = bit_spin(lax.broadcasted_iota(jnp.int32, (8, LANES), 1), 0) * lane_link
    sub = lax.broadcasted_iota(jnp.int32, (CHUNK // 8, 8, LANES), 1)
    odd = (sub & 1) == 1
    second = (sub & 2) == 2
    weights = flips[...]

    def flipped(c, j):
        base = pl.multiple_of(j * CHUNK, CHUNK)
        x = own[0, c, pl.ds(base, CHUNK), :]
        coarse = x.astype(jnp.bfloat16)
        fine = (x - coarse.astype(jnp.float32)).astype(jnp.bfloat16)
        product = jnp.dot(
            jnp.concatenate([coarse, fine], axis=1), weights, preferred_element_type=jnp.float32
        )
        total = product[:, :LANES] + product[:, LANES:]
        x3 = x.reshape(CHUNK // 8, 8, LANES)
        near = jnp.where(odd, pltpu.roll(x3, 1, 1), pltpu.roll(x3, 7, 1))
        middle = jnp.where(second, pltpu.roll(x3, 2, 1), pltpu.roll(x3, 6, 1))
        far = pltpu.roll(x3, 4, 1)
        side = fields[7] * near + fields[8] * middle + fields[9] * far
        total = total + side.reshape(CHUNK, LANES)
        for k in range(3, chunk_bits):
            size = 1 << k
            parts = [
                x[(p ^ 1) * size : ((p ^ 1) + 1) * size] for p in range(CHUNK // size)
            ]
            total = total + fields[7 + k] * jnp.concatenate(parts, axis=0)
        for k in range(chunk_bits, row_bits):
            other = pl.multiple_of((j ^ (1 << (k - chunk_bits))) * CHUNK, CHUNK)
            total = total + fields[7 + k] * own[0, c, pl.ds(other, CHUNK), :]
        for b in range(high_bits):
            total = total + fields[7 + row_bits + b] * partners[b][0, c, pl.ds(base, CHUNK), :]
        return x, total

    def body(j, carry):
        norm, tilt = carry
        base = pl.multiple_of(j * CHUNK, CHUNK)
        count = jnp.int32(0)
        for k in range(row_bits - chunk_bits):
            count = count + (j >> k & 1)
        outer_ones = count.astype(jnp.float32) * (1.0 / spins) + high_ones
        top_spin = 1 - 2 * (j >> (row_bits - chunk_bits - 1) & 1)
        constant = top_spin.astype(jnp.float32) * top_link + high_energy
        real, flip_real = flipped(0, j)
        imag, flip_imag = flipped(1, j)
        shift = inner_ones + (outer_ones - magnet)
        energy = low_energy[pl.ds(base, CHUNK), :].reshape(CHUNK // 8, 8, LANES)
        energy = (energy + (lane_row + constant)[None]).reshape(CHUNK, LANES)
        keep = factor + shift * (kick_one - damp * shift)
        turn = kick_two * shift + rate * energy
        new_real = keep * real - turn * imag - rate * flip_imag
        new_imag = keep * imag + turn * real + rate * flip_real
        out[0, 0, pl.ds(base, CHUNK), :] = new_real
        out[0, 1, pl.ds(base, CHUNK), :] = new_imag
        weight = new_real * new_real + new_imag * new_imag
        tilted = weight * (inner_ones + outer_ones)
        norm = norm + jnp.sum(weight.reshape(CHUNK // 8, 8, LANES), axis=0)
        tilt = tilt + jnp.sum(tilted.reshape(CHUNK // 8, 8, LANES), axis=0)
        return norm, tilt

    zero = jnp.zeros((8, LANES), jnp.float32)
    norm, tilt = lax.fori_loop(0, rows // CHUNK, body, (zero, zero))
    sums[0, 0] = norm
    sums[0, 1] = tilt


def one_step(blocks, table, count, params, block_params, fields, flips, low_energy, high_bits, spins):
    _, _, rows, _ = blocks.shape
    shape = (1, 2, rows, LANES)
    smem = pl.BlockSpec(memory_space=pltpu.SMEM)

    def pick(slot):
        return pl.BlockSpec(shape, lambda g, t: (t[g * (1 + high_bits) + slot], 0, 0, 0))

    grid_spec = pltpu.PrefetchScalarGridSpec(
        num_scalar_prefetch=1,
        grid=(count,),
        in_specs=[
            smem,
            smem,
            smem,
            pl.BlockSpec((2 * LANES, 2 * LANES), lambda g, t: (0, 0)),
            pl.BlockSpec((rows, LANES), lambda g, t: (0, 0)),
        ]
        + [pick(slot) for slot in range(1 + high_bits)],
        out_specs=[
            pl.BlockSpec(shape, lambda g, t: (g, 0, 0, 0)),
            pl.BlockSpec((1, 2, 8, LANES), lambda g, t: (g, 0, 0, 0)),
        ],
    )
    return pl.pallas_call(
        functools.partial(step_kernel, high_bits, spins),
        grid_spec=grid_spec,
        out_shape=[
            jax.ShapeDtypeStruct((count, 2, rows, LANES), jnp.float32),
            jax.ShapeDtypeStruct((count, 2, 8, LANES), jnp.float32),
        ],
        compiler_params=pltpu.CompilerParams(vmem_limit_bytes=58 << 20),
    )(table, params, block_params, fields, flips, low_energy, *([blocks] * (1 + high_bits)))


def shards(state, fields, couplings, noise):
    local_len = state.shape[2]
    low_bits = local_len.bit_length() - 1
    blocks_all = lax.axis_size("gx")
    high_bits = blocks_all.bit_length() - 1
    spins = low_bits + high_bits
    steps = noise.shape[1]
    rows = local_len // LANES
    me = lax.axis_index("gx")
    f32 = jnp.float32

    order = sorted(range(blocks_all), key=lambda p: (bin(p).count("1"), p))
    place = {p: g for g, p in enumerate(order)}

    x = state.reshape(2, rows, LANES)
    row_ids = lax.broadcasted_iota(jnp.int32, (rows, LANES), 0)
    lane_ids = lax.broadcasted_iota(jnp.int32, (rows, LANES), 1)
    position = row_ids * LANES + lane_ids
    low_energy = jnp.zeros((rows, LANES), f32)
    occupancy = jnp.zeros((rows, LANES), jnp.int32)
    for q in range(low_bits):
        occupancy = occupancy + (position >> q & 1)
    for q in range(low_bits - 1):
        low_energy = low_energy + couplings[q] * bit_spin(position, q) * bit_spin(position, q + 1)
    own_ones = lax.population_count(me)
    weight = x[0] * x[0] + x[1] * x[1]
    start = jnp.stack(
        [
            jnp.sum(weight),
            jnp.sum(weight * ((occupancy + own_ones).astype(f32) * (1.0 / spins))),
        ]
    )
    totals = lax.psum(start, "gx")

    ids = lax.iota(jnp.int32, LANES)
    distance = ids[:, None] ^ ids[None, :]
    lane_flip = jnp.zeros((LANES, LANES), f32)
    for q in range(7):
        lane_flip = lane_flip + fields[q] * (distance == 1 << q).astype(f32)
    coarse = lax.reduce_precision(lane_flip, 8, 7)
    fine = (lane_flip - coarse).astype(jnp.bfloat16)
    coarse = coarse.astype(jnp.bfloat16)
    flips = jnp.concatenate(
        [
            jnp.concatenate([coarse, fine], axis=1),
            jnp.concatenate([coarse, jnp.zeros_like(fine)], axis=1),
        ],
        axis=0,
    )

    targets = me ^ jnp.array(order, jnp.int32)
    high_spin = [bit_spin(targets, b) for b in range(high_bits)]
    high_energy = jnp.zeros((blocks_all,), f32)
    for b in range(high_bits - 1):
        high_energy = high_energy + couplings[low_bits + b] * high_spin[b] * high_spin[b + 1]
    block_params = jnp.stack(
        [
            lax.population_count(targets).astype(f32) * (1.0 / spins),
            couplings[low_bits - 1] * high_spin[0],
            couplings[spins - 1] * high_spin[-1],
            high_energy,
        ],
        axis=1,
    ).reshape(-1)

    blocks = lax.all_gather(x, "gx")
    half_root = jnp.sqrt(f32(time_step / 2.0))
    root_kappa = jnp.sqrt(f32(kappa_rate))
    records = []
    for s in range(steps):
        reach = steps - 1 - s
        count = sum(bin(p).count("1") <= reach for p in order)
        if blocks_all - count <= 1:
            count = blocks_all
        table = [[place[order[g]]] + [place[order[g] ^ 1 << b] for b in range(high_bits)] for g in range(count)]
        if s == 0:
            absolute = [[order[slot] for slot in entry] for entry in table]
            table = me ^ jnp.array(absolute, jnp.int32).reshape(-1)
        else:
            table = jnp.array(table, jnp.int32).reshape(-1)
        magnet = totals[1] / totals[0]
        factor = jnp.sqrt(f32(local_len * blocks_all) / totals[0])
        first = noise[0, s, 0] * half_root
        second = noise[0, s, 1] * half_root
        params = jnp.stack(
            [
                factor * time_step,
                factor,
                factor * (time_step * kappa_rate * 0.5),
                factor * root_kappa * first,
                factor * root_kappa * second,
                magnet,
            ]
        )
        drift = root_kappa * magnet * time_step
        records.append(jnp.stack([drift + first, drift + second]))
        blocks, sums = one_step(
            blocks, table, count, params, block_params, fields, flips, low_energy, high_bits, spins
        )
        if s < steps - 1:
            if count == blocks_all:
                totals = jnp.sum(sums, axis=(0, 2, 3))
            else:
                totals = lax.psum(jnp.sum(sums[0], axis=(1, 2)), "gx")
    local = jnp.where(me == 0, jnp.stack(records), 0.0)
    record = lax.psum(local, ("gx", "gy"))
    return blocks.reshape(1, 2, local_len), record


def solution(mesh):
    placed = (P("gy", None, "gx"), P(), P(), P("gy", None, None))
    return jax.shard_map(
        shards, mesh=mesh, in_specs=placed, out_specs=(P("gy", None, "gx"), P()), check_vma=False
    )
```

```python
import functools

import jax
import jax.numpy as jnp
from jax import lax
from jax.experimental import pallas as pl
from jax.experimental.pallas import tpu as pltpu
from jax.sharding import PartitionSpec as P

kappa_rate = 4.0
time_step = 0.05
LANES = 128
CHUNK = 64


def bit_spin(ids, q):
    return 1.0 - 2.0 * (ids >> q & 1).astype(jnp.float32)


def step_kernel(
    high_bits, spins, table, params, block_params, fields, flips, low_energy, own, *rest
):
    partners = rest[:high_bits]
    out, sums = rest[high_bits:]
    rows = own.shape[2]
    row_bits = rows.bit_length() - 1
    chunk_bits = CHUNK.bit_length() - 1
    g = pl.program_id(0)
    rate, factor, damp, kick_one, kick_two, magnet = (params[k] for k in range(6))
    high_ones, top_link, lane_link, high_energy = (block_params[g * 4 + k] for k in range(4))

    row_ids = lax.broadcasted_iota(jnp.int32, (CHUNK, LANES), 0)
    lane_ids = lax.broadcasted_iota(jnp.int32, (CHUNK, LANES), 1)
    ones = jnp.zeros((CHUNK, LANES), jnp.int32)
    for k in range(7):
        ones = ones + (lane_ids >> k & 1)
    for k in range(chunk_bits):
        ones = ones + (row_ids >> k & 1)
    inner_ones = ones.astype(jnp.float32) * (1.0 / spins)
    lane_row = bit_spin(lax.broadcasted_iota(jnp.int32, (8, LANES), 1), 0) * lane_link
    sub = lax.broadcasted_iota(jnp.int32, (CHUNK // 8, 8, LANES), 1)
    odd = (sub & 1) == 1
    second = (sub & 2) == 2
    weights = flips[...]

    def flipped(c, j):
        base = pl.multiple_of(j * CHUNK, CHUNK)
        x = own[0, c, pl.ds(base, CHUNK), :]
        coarse = x.astype(jnp.bfloat16)
        fine = (x - coarse.astype(jnp.float32)).astype(jnp.bfloat16)
        product = jnp.dot(
            jnp.concatenate([coarse, fine], axis=1), weights, preferred_element_type=jnp.float32
        )
        total = product[:, :LANES] + product[:, LANES:]
        x3 = x.reshape(CHUNK // 8, 8, LANES)
        near = jnp.where(odd, pltpu.roll(x3, 1, 1), pltpu.roll(x3, 7, 1))
        middle = jnp.where(second, pltpu.roll(x3, 2, 1), pltpu.roll(x3, 6, 1))
        far = pltpu.roll(x3, 4, 1)
        side = fields[7] * near + fields[8] * middle + fields[9] * far
        total = total + side.reshape(CHUNK, LANES)
        for k in range(3, chunk_bits):
            size = 1 << k
            parts = [
                x[(p ^ 1) * size : ((p ^ 1) + 1) * size] for p in range(CHUNK // size)
            ]
            total = total + fields[7 + k] * jnp.concatenate(parts, axis=0)
        for k in range(chunk_bits, row_bits):
            other = pl.multiple_of((j ^ (1 << (k - chunk_bits))) * CHUNK, CHUNK)
            total = total + fields[7 + k] * own[0, c, pl.ds(other, CHUNK), :]
        for b in range(high_bits):
            total = total + fields[7 + row_bits + b] * partners[b][0, c, pl.ds(base, CHUNK), :]
        return x, total

    def body(j, carry):
        norm, tilt = carry
        base = pl.multiple_of(j * CHUNK, CHUNK)
        count = jnp.int32(0)
        for k in range(row_bits - chunk_bits):
            count = count + (j >> k & 1)
        outer_ones = count.astype(jnp.float32) * (1.0 / spins) + high_ones
        top_spin = 1 - 2 * (j >> (row_bits - chunk_bits - 1) & 1)
        constant = top_spin.astype(jnp.float32) * top_link + high_energy
        real, flip_real = flipped(0, j)
        imag, flip_imag = flipped(1, j)
        shift = inner_ones + (outer_ones - magnet)
        energy = low_energy[pl.ds(base, CHUNK), :].reshape(CHUNK // 8, 8, LANES)
        energy = (energy + (lane_row + constant)[None]).reshape(CHUNK, LANES)
        keep = factor + shift * (kick_one - damp * shift)
        turn = kick_two * shift + rate * energy
        new_real = keep * real - turn * imag - rate * flip_imag
        new_imag = keep * imag + turn * real + rate * flip_real
        out[0, 0, pl.ds(base, CHUNK), :] = new_real
        out[0, 1, pl.ds(base, CHUNK), :] = new_imag
        weight = new_real * new_real + new_imag * new_imag
        tilted = weight * (inner_ones + outer_ones)
        norm = norm + jnp.sum(weight.reshape(CHUNK // 8, 8, LANES), axis=0)
        tilt = tilt + jnp.sum(tilted.reshape(CHUNK // 8, 8, LANES), axis=0)
        return norm, tilt

    zero = jnp.zeros((8, LANES), jnp.float32)
    norm, tilt = lax.fori_loop(0, rows // CHUNK, body, (zero, zero))
    sums[0, 0] = norm
    sums[0, 1] = tilt


def one_step(blocks, table, count, params, block_params, fields, flips, low_energy, high_bits, spins):
    _, _, rows, _ = blocks.shape
    shape = (1, 2, rows, LANES)
    smem = pl.BlockSpec(memory_space=pltpu.SMEM)

    def pick(slot):
        return pl.BlockSpec(shape, lambda g, t: (t[g * (1 + high_bits) + slot], 0, 0, 0))

    grid_spec = pltpu.PrefetchScalarGridSpec(
        num_scalar_prefetch=1,
        grid=(count,),
        in_specs=[
            smem,
            smem,
            smem,
            pl.BlockSpec((2 * LANES, 2 * LANES), lambda g, t: (0, 0)),
            pl.BlockSpec((rows, LANES), lambda g, t: (0, 0)),
        ]
        + [pick(slot) for slot in range(1 + high_bits)],
        out_specs=[
            pl.BlockSpec(shape, lambda g, t: (g, 0, 0, 0)),
            pl.BlockSpec((1, 2, 8, LANES), lambda g, t: (g, 0, 0, 0)),
        ],
    )
    return pl.pallas_call(
        functools.partial(step_kernel, high_bits, spins),
        grid_spec=grid_spec,
        out_shape=[
            jax.ShapeDtypeStruct((count, 2, rows, LANES), jnp.float32),
            jax.ShapeDtypeStruct((count, 2, 8, LANES), jnp.float32),
        ],
        compiler_params=pltpu.CompilerParams(vmem_limit_bytes=58 << 20),
    )(table, params, block_params, fields, flips, low_energy, *([blocks] * (1 + high_bits)))


def shards(state, fields, couplings, noise):
    local_len = state.shape[2]
    low_bits = local_len.bit_length() - 1
    blocks_all = lax.axis_size("gx")
    high_bits = blocks_all.bit_length() - 1
    spins = low_bits + high_bits
    steps = noise.shape[1]
    rows = local_len // LANES
    me = lax.axis_index("gx")
    f32 = jnp.float32

    order = sorted(range(blocks_all), key=lambda p: (bin(p).count("1"), p))
    place = {p: g for g, p in enumerate(order)}

    x = state.reshape(2, rows, LANES)
    row_ids = lax.broadcasted_iota(jnp.int32, (rows, LANES), 0)
    lane_ids = lax.broadcasted_iota(jnp.int32, (rows, LANES), 1)
    position = row_ids * LANES + lane_ids
    low_energy = jnp.zeros((rows, LANES), f32)
    occupancy = jnp.zeros((rows, LANES), jnp.int32)
    for q in range(low_bits):
        occupancy = occupancy + (position >> q & 1)
    for q in range(low_bits - 1):
        low_energy = low_energy + couplings[q] * bit_spin(position, q) * bit_spin(position, q + 1)
    own_ones = lax.population_count(me)
    weight = x[0] * x[0] + x[1] * x[1]
    start = jnp.stack(
        [
            jnp.sum(weight),
            jnp.sum(weight * ((occupancy + own_ones).astype(f32) * (1.0 / spins))),
        ]
    )
    totals = lax.psum(start, "gx")

    ids = lax.iota(jnp.int32, LANES)
    distance = ids[:, None] ^ ids[None, :]
    lane_flip = jnp.zeros((LANES, LANES), f32)
    for q in range(7):
        lane_flip = lane_flip + fields[q] * (distance == 1 << q).astype(f32)
    coarse = lax.reduce_precision(lane_flip, 8, 7)
    fine = (lane_flip - coarse).astype(jnp.bfloat16)
    coarse = coarse.astype(jnp.bfloat16)
    flips = jnp.concatenate(
        [
            jnp.concatenate([coarse, fine], axis=1),
            jnp.concatenate([coarse, jnp.zeros_like(fine)], axis=1),
        ],
        axis=0,
    )

    targets = me ^ jnp.array(order, jnp.int32)
    high_spin = [bit_spin(targets, b) for b in range(high_bits)]
    high_energy = jnp.zeros((blocks_all,), f32)
    for b in range(high_bits - 1):
        high_energy = high_energy + couplings[low_bits + b] * high_spin[b] * high_spin[b + 1]
    block_params = jnp.stack(
        [
            lax.population_count(targets).astype(f32) * (1.0 / spins),
            couplings[low_bits - 1] * high_spin[0],
            couplings[spins - 1] * high_spin[-1],
            high_energy,
        ],
        axis=1,
    ).reshape(-1)

    ring = list(range(0, blocks_all, 2)) + list(range(blocks_all - 1, 0, -2))
    ahead = [(ring[i - 1], ring[i]) for i in range(blocks_all)]
    back = [(target, source) for source, target in ahead]
    half = blocks_all // 2
    slots = [None] * blocks_all
    slots[0] = x
    from_back = from_ahead = x
    for hop in range(1, half):
        from_back = lax.ppermute(from_back, "gx", ahead)
        from_ahead = lax.ppermute(from_ahead, "gx", back)
        slots[hop] = from_back
        slots[blocks_all - hop] = from_ahead
    slots[half] = jnp.concatenate(
        [lax.ppermute(from_back[:1], "gx", ahead), lax.ppermute(from_ahead[1:], "gx", back)]
    )
    blocks = jnp.stack(slots)

    def ring_place(i):
        return jnp.where(i & 1 == 1, blocks_all - 1 - (i >> 1), i >> 1)

    half_root = jnp.sqrt(f32(time_step / 2.0))
    root_kappa = jnp.sqrt(f32(kappa_rate))
    records = []
    for s in range(steps):
        reach = steps - 1 - s
        count = sum(bin(p).count("1") <= reach for p in order)
        if blocks_all - count <= 1:
            count = blocks_all
        table = [[place[order[g]]] + [place[order[g] ^ 1 << b] for b in range(high_bits)] for g in range(count)]
        if s == 0:
            absolute = [[order[slot] for slot in entry] for entry in table]
            target = me ^ jnp.array(absolute, jnp.int32).reshape(-1)
            table = (ring_place(me) - ring_place(target)) & (blocks_all - 1)
        else:
            table = jnp.array(table, jnp.int32).reshape(-1)
        magnet = totals[1] / totals[0]
        factor = jnp.sqrt(f32(local_len * blocks_all) / totals[0])
        first = noise[0, s, 0] * half_root
        second = noise[0, s, 1] * half_root
        params = jnp.stack(
            [
                factor * time_step,
                factor,
                factor * (time_step * kappa_rate * 0.5),
                factor * root_kappa * first,
                factor * root_kappa * second,
                magnet,
            ]
        )
        drift = root_kappa * magnet * time_step
        records.append(jnp.stack([drift + first, drift + second]))
        blocks, sums = one_step(
            blocks, table, count, params, block_params, fields, flips, low_energy, high_bits, spins
        )
        if s < steps - 1:
            if count == blocks_all:
                totals = jnp.sum(sums, axis=(0, 2, 3))
            else:
                totals = lax.psum(jnp.sum(sums[0], axis=(1, 2)), "gx")
    local = jnp.where(me == 0, jnp.stack(records), 0.0)
    record = lax.psum(local, ("gx", "gy"))
    return blocks.reshape(1, 2, local_len), record


def solution(mesh):
    placed = (P("gy", None, "gx"), P(), P(), P("gy", None, None))
    return jax.shard_map(
        shards, mesh=mesh, in_specs=placed, out_specs=(P("gy", None, "gx"), P()), check_vma=False
    )
```
